32 devices in a mesh: gx: 4 (over y, core), gy: 8 (over z, x).
Axes of the slice: x: 2, y: 2, z: 4, core: 2. Of those that a mesh axis runs over, the one named last changes fastest.
Arguments:
- particle_cell: int32 [4, 8, 65536], P('gx', 'gy'), may hold values from -1 to 16383, as said below
- particle_mass: float32 [4, 8, 65536], P('gx', 'gy'), may hold values from 0.5 to 2
Outputs:
- potential: float32 [64, 64, 128], P('gx', 'gy')
- residual: float32 [64, 64, 128], P('gx', 'gy')
- residual_norms: float32 [2], replicated
The draws below stay inside these ranges and needn't reach their ends.
Inputs may be any that keep to these rules, and one draw needn't show every extreme that they name: `particle_cell`: -1 marks an empty slot; any other value v names the cell (v // 1024, v // 128 % 8, v % 128) of the block of 16 x 8 x 128 cells that belongs to the slot's tile.
All inputs are finite; a program needn't handle non-finite values.
Results may differ from the reference program's by a relative error of at most 0.0003.
Values sent between devices are 32-bit elements; how exact they have to be, the bound alone decides.
A program may use at most 64 MiB of HBM per device.

```python
import math
import jax
import jax.numpy as jnp

CX = 16
CY = 8
NZ = 128
P_DEV = 65536
LEVELS = 4
CYCLES = 2
COARSE_SWEEPS = 2
TILES_X = 4
TILES_Y = 8
NX = 64
NY = 64


def shuffled_ranks(subkey):
    return jax.random.permutation(subkey, P_DEV)


def draw_particle_cell(key, part):
    tile_count = TILES_X * TILES_Y
    block_cells = CX * CY * NZ
    base = jax.random.fold_in(key, 11)
    key_cell, key_keep, key_jitter = jax.random.split(base, 3)
    placed = jax.random.randint(key_cell, (tile_count, P_DEV), 0, block_cells, dtype=jnp.int32)
    order = jnp.arange(tile_count, dtype=jnp.int32)
    span_tiles = max(tile_count - 1, 1)
    occupied_count = P_DEV - 2 * P_DEV // 3 * (tile_count - 1 - order) // span_tiles
    jitter = jax.random.randint(key_jitter, (tile_count,), 0, P_DEV // 8 + 1, dtype=jnp.int32)
    occupied_count = occupied_count - jnp.where(order == tile_count - 1, 0, jitter)
    ranks = jax.vmap(shuffled_ranks)(jax.random.split(key_keep, tile_count)).astype(jnp.int32)
    chosen = jnp.where(ranks < occupied_count[:, None], placed, -1)
    return chosen.reshape(TILES_X, TILES_Y, P_DEV).astype(jnp.int32)


def shard_levels(key, shape, shards, smallest, largest):
    gain, own = 1.0, jax.random.fold_in(key, 6)
    for position, shards_of in shards:
        heights = jnp.exp(jax.random.uniform(jax.random.fold_in(own, position), (shards_of,), jnp.float32, smallest / len(shards), largest / len(shards)))
        gain = gain * jnp.repeat(heights, shape[position] // shards_of).reshape([-1 if axis == position else 1 for axis in range(len(shape))])
    return gain


def setup_inputs(seed: int = 0) -> dict:
    streams_of = jax.random.split(jax.random.key(seed), 3)
    particle_cell = draw_particle_cell(jax.random.fold_in(streams_of[2], 71), 0)
    particle_mass = jnp.clip(jnp.exp(math.log(2.0) - 1.3862944 * jax.random.uniform(streams_of[1], (TILES_X, TILES_Y, P_DEV), jnp.float32) ** shard_levels(streams_of[1], (TILES_X, TILES_Y, P_DEV), ((0, 4), (1, 8)), -0.2, 0.2)), 0.5, 2.0)
    return {"particle_cell": particle_cell, "particle_mass": particle_mass}


coupling = 0.03125
norm_eps = 1e-06

def roll_sum(values):
    beside = jnp.roll(values, 1, 0) + jnp.roll(values, -1, 0)
    beside = beside + jnp.roll(values, 1, 1) + jnp.roll(values, -1, 1)
    return beside + jnp.roll(values, 1, 2) + jnp.roll(values, -1, 2)

def parity_mask(shape):
    index_x = jnp.arange(shape[0], dtype=jnp.int32)[:, None, None]
    index_y = jnp.arange(shape[1], dtype=jnp.int32)[None, :, None]
    index_z = jnp.arange(shape[2], dtype=jnp.int32)[None, None, :]
    return (index_x + index_y + index_z) % 2 == 0

def whole_sweep(estimate, source, spacing_squared, red_cells):
    updated = (roll_sum(estimate) + spacing_squared * source) / 6.0
    estimate = jnp.where(red_cells, updated, estimate)
    updated = (roll_sum(estimate) + spacing_squared * source) / 6.0
    return jnp.where(red_cells, estimate, updated)

def whole_residual(estimate, source, spacing_squared):
    return source - (6.0 * estimate - roll_sum(estimate)) / spacing_squared

def restrict(values):
    rows_x, rows_y, rows_z = values.shape
    return values.reshape(rows_x // 2, 2, rows_y // 2, 2, rows_z // 2, 2).mean(axis=(1, 3, 5))

def prolong(values):
    rows_x, rows_y, rows_z = values.shape
    spread = jnp.broadcast_to(values[:, None, :, None, :, None], (rows_x, 2, rows_y, 2, rows_z, 2))
    return spread.reshape(2 * rows_x, 2 * rows_y, 2 * rows_z)

def whole_cycle(grid_level, estimate, source):
    spacing_squared = float(4 ** grid_level)
    red_cells = parity_mask(estimate.shape)
    if grid_level == LEVELS - 1:
        for repeat in range(COARSE_SWEEPS):
            estimate = whole_sweep(estimate, source, spacing_squared, red_cells)
        return estimate
    estimate = whole_sweep(estimate, source, spacing_squared, red_cells)
    coarse_source = restrict(whole_residual(estimate, source, spacing_squared))
    correction = whole_cycle(grid_level + 1, jnp.zeros_like(coarse_source), coarse_source)
    estimate = estimate + prolong(correction)
    return whole_sweep(estimate, source, spacing_squared, red_cells)

def reference(particle_cell, particle_mass):
    grid_cells = NX * NY * NZ
    local_x = particle_cell // (CY * NZ)
    local_y = particle_cell // NZ % CY
    local_z = particle_cell % NZ
    tile_x = jnp.arange(TILES_X, dtype=jnp.int32)[:, None, None]
    tile_y = jnp.arange(TILES_Y, dtype=jnp.int32)[None, :, None]
    flat_index = ((tile_x * CX + local_x) * NY + tile_y * CY + local_y) * NZ + local_z
    occupied = particle_cell >= 0
    flat_index = jnp.where(occupied, flat_index, grid_cells).astype(jnp.int32)
    density = jnp.zeros((grid_cells + 1,), jnp.float32).at[flat_index.reshape(-1)].add(particle_mass.reshape(-1))
    density = density[:grid_cells].reshape(NX, NY, NZ)
    total_mass = jnp.sum(jnp.where(occupied, particle_mass, 0.0))
    mean_mass = total_mass / grid_cells
    source = coupling * (1.0 - density / mean_mass)
    estimate = jnp.zeros((NX, NY, NZ), jnp.float32)
    norm_list = []
    residual = source
    for cycle_index in range(CYCLES):
        estimate = whole_cycle(0, estimate, source)
        residual = whole_residual(estimate, source, 1.0) / coupling
        norm_list.append(jnp.sqrt(jnp.sum(residual * residual) / grid_cells + norm_eps))
    return (estimate, residual, jnp.stack(norm_list))
```

```python
import functools

import jax
import jax.numpy as jnp
from jax import lax
from jax.experimental import pallas as pl
from jax.experimental.pallas import tpu as pltpu
from jax.sharding import PartitionSpec as P

CX = 16
CY = 8
NZ = 128
LEVELS = 4
CYCLES = 2
COARSE_SWEEPS = 2
HALO = 8

coupling = 0.03125
norm_eps = 1e-06

MESH = pl.DeviceIdType.MESH
F32 = jnp.float32
BF16 = jnp.bfloat16


def deposit_kernel(cell_ref, mass_ref, density_ref, sums_ref, acc_ref, msum_ref):
    rows = cell_ref.shape[0]
    step = 8
    cells = CX * CY
    acc_ref[...] = jnp.zeros_like(acc_ref)
    msum_ref[...] = jnp.zeros_like(msum_ref)

    def body(i, carry):
        at = pl.ds(pl.multiple_of(i * step, step), step)
        slot = cell_ref[at, :]
        mass = jnp.where(slot >= 0, mass_ref[at, :], 0.0)
        msum_ref[...] += mass
        high = mass.astype(BF16).astype(F32)
        rest = mass - high
        middle = rest.astype(BF16).astype(F32)
        low = rest - middle
        row = slot >> 7
        z = slot & (NZ - 1)
        row_ids = lax.broadcasted_iota(jnp.int32, (cells, 128), 0)
        z_ids = lax.broadcasted_iota(jnp.int32, (NZ, 128), 0)
        left, right = [], []
        for k in range(step):
            hit = row_ids == jnp.broadcast_to(row[k : k + 1], (cells, 128))
            pieces = [
                jnp.where(hit, jnp.broadcast_to(piece[k : k + 1], (cells, 128)), 0.0).astype(BF16)
                for piece in (high, middle, low)
            ]
            left.append(jnp.concatenate(pieces, axis=0))
            there = z_ids == jnp.broadcast_to(z[k : k + 1], (NZ, 128))
            right.append(jnp.where(there, 1.0, 0.0).astype(BF16))
        acc_ref[...] += lax.dot_general(
            jnp.concatenate(left, axis=1),
            jnp.concatenate(right, axis=1),
            (((1,), (1,)), ((), ())),
            preferred_element_type=F32,
        )
        return carry

    lax.fori_loop(0, rows // step, body, 0)
    density_ref[...] = acc_ref[0:cells] + (acc_ref[cells : 2 * cells] + acc_ref[2 * cells :])
    sums_ref[...] = jnp.sum(msum_ref[...], axis=0, keepdims=True)


def colour_of(shape, level):
    x = lax.broadcasted_iota(jnp.int32, shape, 0)
    y = lax.broadcasted_iota(jnp.int32, shape, 1)
    z = lax.broadcasted_iota(jnp.int32, shape, 2) >> level
    return (x + y + z) & 1


def chunk_of(planes, rows_y):
    chunk = 2
    while 2 * chunk * rows_y <= 128 and planes % (2 * chunk) == 0:
        chunk *= 2
    return chunk


def neighbours(u_ref, x0, chunk, level):
    planes, rows_y, lanes = u_ref.shape
    centre = u_ref[pl.ds(x0, chunk)]
    if chunk == planes:
        before, after = centre[planes - 1 :], centre[:1]
    else:
        before = u_ref[pl.ds(lax.rem(x0 + planes - 1, planes), 1)]
        after = u_ref[pl.ds(lax.rem(x0 + chunk, planes), 1)]
    total = jnp.concatenate([before, centre[:-1]], axis=0)
    total += jnp.concatenate([centre[1:], after], axis=0)
    total += pltpu.roll(centre, 1, 1) + pltpu.roll(centre, rows_y - 1, 1)
    stride = 2**level
    total += pltpu.roll(centre, stride, 2) + pltpu.roll(centre, lanes - stride, 2)
    return centre, total


def over_planes(planes, chunk, body, start=0):
    if planes == chunk:
        body(start)
        return

    def step(i, carry):
        body(start + i * chunk)
        return carry

    lax.fori_loop(0, planes // chunk, step, 0)


def relax(u_ref, b_ref, level, wanted):
    planes, rows_y, lanes = u_ref.shape
    chunk = chunk_of(planes, rows_y)
    spacing = float(4**level)

    def body(x0):
        centre, total = neighbours(u_ref, x0, chunk, level)
        new = (total + spacing * b_ref[pl.ds(x0, chunk)]) * (1.0 / 6.0)
        u_ref[pl.ds(x0, chunk)] = jnp.where(colour_of(centre.shape, level) == wanted, new, centre)

    over_planes(planes, chunk, body)


def sweep(u_ref, b_ref, level):
    relax(u_ref, b_ref, level, 0)
    relax(u_ref, b_ref, level, 1)


def first_sweep(u_ref, b_ref, level):
    planes, rows_y, lanes = u_ref.shape
    chunk = chunk_of(planes, rows_y)
    scale = float(4**level) / 6.0

    def body(x0):
        b = b_ref[pl.ds(x0, chunk)]
        u_ref[pl.ds(x0, chunk)] = jnp.where(colour_of(b.shape, level) == 0, b * scale, 0.0)

    over_planes(planes, chunk, body)
    relax(u_ref, b_ref, level, 1)


def pair_means(u_ref, b_ref, tmp_ref, level, x0, chunk):
    centre, total = neighbours(u_ref, x0, chunk, level)
    res = b_ref[pl.ds(x0, chunk)] - (6.0 * centre - total) * (1.0 / float(4**level))
    rows_y, lanes = res.shape[1:]
    pairs = res.reshape(chunk // 2, 2, rows_y, lanes)
    along_x = pairs[:, 0] + pairs[:, 1]
    stride = 2**level
    bit = (lax.broadcasted_iota(jnp.int32, along_x.shape, 2) >> level) & 1
    other = jnp.where(
        bit == 0, pltpu.roll(along_x, lanes - stride, 2), pltpu.roll(along_x, stride, 2)
    )
    tmp_ref[0 : chunk // 2, 0:rows_y, :] = (along_x + other) * 0.125


def y_pairs(tmp_ref, count, start, rows):
    return tmp_ref[0:count, pl.ds(start, rows, 2), :] + tmp_ref[0:count, pl.ds(start + 1, rows, 2), :]


def restrict(u_ref, b_ref, tmp_ref, coarse_ref, level):
    planes, rows_y, _ = u_ref.shape
    chunk = chunk_of(planes, rows_y)

    def body(x0):
        pair_means(u_ref, b_ref, tmp_ref, level, x0, chunk)
        coarse_ref[pl.ds(x0 // 2, chunk // 2)] = y_pairs(tmp_ref, chunk // 2, 0, rows_y // 2)

    over_planes(planes, chunk, body)


def spread_add(u_ref, coarse, tmp_ref, x0, chunk):
    half, rows, lanes = coarse.shape
    tmp_ref[0:half, pl.ds(0, rows, 2), :] = coarse
    tmp_ref[0:half, pl.ds(1, rows, 2), :] = coarse
    wide = tmp_ref[0:half, 0 : 2 * rows, :]
    wide = jnp.broadcast_to(wide[:, None], (half, 2, 2 * rows, lanes))
    u_ref[pl.ds(x0, chunk)] += wide.reshape(chunk, 2 * rows, lanes)


def prolong_add(u_ref, coarse_ref, tmp_ref):
    planes, rows_y, _ = u_ref.shape
    chunk = chunk_of(planes, rows_y)

    def body(x0):
        spread_add(u_ref, coarse_ref[pl.ds(x0 // 2, chunk // 2)], tmp_ref, x0, chunk)

    over_planes(planes, chunk, body)


def main_kernel(tiles_x, tiles_y, density_ref, sums_ref, potential_ref, residual_ref, norms_ref, *scratch):
    count = tiles_x * tiles_y
    (ext, b0, u0, mass_buf, norm_buf, norm_msg, packed, gathered, tmp) = scratch[:9]
    fields = scratch[9 : 9 + 2 * (LEVELS - 1)]
    halo_send, halo_recv, all_send, all_recv = scratch[9 + 2 * (LEVELS - 1) :]
    tile_x = lax.axis_index("gx")
    tile_y = lax.axis_index("gy")
    me = tile_x * tiles_y + tile_y
    grid_cells = CX * CY * NZ * count
    b = [b0] + [fields[2 * i] for i in range(LEVELS - 1)]
    u = [u0] + [fields[2 * i + 1] for i in range(LEVELS - 1)]

    def partner(k):
        d = lax.rem(me + k, count)
        return (d // tiles_y, lax.rem(d, tiles_y))

    barrier = pltpu.get_barrier_semaphore()

    def greet(k, carry):
        pl.semaphore_signal(barrier, inc=1, device_id=partner(k), device_id_type=MESH)
        return carry

    lax.fori_loop(1, count, greet, 0)
    pl.semaphore_wait(barrier, count - 1)

    def to_all(src, dst, which):
        def send(k, carry):
            pltpu.make_async_remote_copy(
                src_ref=src,
                dst_ref=dst.at[me],
                send_sem=all_send.at[which],
                recv_sem=all_recv.at[which],
                device_id=partner(k),
                device_id_type=MESH,
            ).start()
            return carry

        lax.fori_loop(1, count, send, 0)

    def from_all(dst, which):
        part = dst.at[pl.ds(0, count - 1)]
        pltpu.make_async_copy(part, part, all_recv.at[which]).wait()
        pltpu.make_async_copy(part, part, all_send.at[which]).wait()

    to_all(sums_ref, mass_buf, 0)
    halos = []
    for dx, dy in ((0, 1), (0, -1), (1, 1), (-1, 1), (1, -1), (-1, -1), (1, 0), (-1, 0)):
        rows = {1: (CX - HALO, HALO, 0), 0: (0, CX, HALO), -1: (0, HALO, HALO + CX)}[dx]
        to_y = {1: 0, 0: HALO, -1: HALO + CY}[dy]
        copy = pltpu.make_async_remote_copy(
            src_ref=density_ref.at[pl.ds(rows[0], rows[1])],
            dst_ref=ext.at[pl.ds(rows[2], rows[1]), pl.ds(to_y, CY), :],
            send_sem=halo_send.at[len(halos)],
            recv_sem=halo_recv.at[len(halos)],
            device_id=(
                lax.rem(tile_x + dx + tiles_x, tiles_x),
                lax.rem(tile_y + dy + tiles_y, tiles_y),
            ),
            device_id_type=MESH,
        )
        copy.start()
        halos.append(copy)
    ext[HALO : HALO + CX, HALO : HALO + CY, :] = density_ref[...]
    mass_buf[me] = sums_ref[...]
    from_all(mass_buf, 0)
    total_mass = jnp.sum(jnp.sum(mass_buf[...], axis=0), axis=-1, keepdims=True)
    scale = coupling / (total_mass / grid_cells)
    for copy in halos:
        copy.wait()

    planes0, rows0, _ = ext.shape
    chunk0 = 4

    def set_source(x0):
        at = pl.ds(x0, chunk0)
        b0[at] = coupling - ext[at] * jnp.broadcast_to(scale.reshape(1, 1, 1), (chunk0, rows0, NZ))

    over_planes(planes0, chunk0, set_source)

    lane = lax.broadcasted_iota(jnp.int32, (1, 1, NZ), 2) & 1
    half_x, half_y = CX // 2, CY // 2

    def coarse_correction(cycle_index):
        slot = packed.at[cycle_index]
        blocks = gathered.at[cycle_index]
        for part in range(CX // chunk0):
            pair_means(u0, b0, tmp, 0, HALO + part * chunk0, chunk0)
            b1_part = y_pairs(tmp, chunk0 // 2, HALO, half_y)
            for j in range(chunk0 // 2):
                plane = part * (chunk0 // 2) + j
                inner = plane % 4
                at = (inner % 2, slice(half_y * (inner // 2), half_y * (inner // 2 + 1)))
                if plane < 4:
                    packed[cycle_index, at[0], at[1], :] = b1_part[j]
                else:
                    old = packed[cycle_index, at[0], at[1], :]
                    packed[cycle_index, at[0], at[1], :] = jnp.where(lane[0] == 0, old, b1_part[j])
        to_all(slot, blocks, 1 + cycle_index)
        gathered[cycle_index, me] = packed[cycle_index]
        from_all(blocks, 1 + cycle_index)

        def unpack(i, carry):
            ix = i // (tiles_y // 2)
            iy = lax.rem(i, tiles_y // 2)
            first = gathered[cycle_index, ix * tiles_y + 2 * iy]
            second = gathered[cycle_index, ix * tiles_y + 2 * iy + 1]
            rows = pl.ds(pl.multiple_of(iy * 8, 8), 8)
            low = jnp.concatenate([first[:, :half_y], second[:, :half_y]], axis=1)
            high = jnp.concatenate([first[:, half_y:], second[:, half_y:]], axis=1)
            for offset, part in ((0, low), (2, high)):
                even = jnp.where(lane == 0, part, pltpu.roll(part, 1, 2))
                odd = jnp.where(lane == 1, part, pltpu.roll(part, NZ - 1, 2))
                b[1][pl.ds(ix * half_x + offset, 2), rows, :] = even
                b[1][pl.ds(ix * half_x + 4 + offset, 2), rows, :] = odd
            return carry

        lax.fori_loop(0, count // 2, unpack, 0)
        for level in range(1, LEVELS):
            first_sweep(u[level], b[level], level)
            if level < LEVELS - 1:
                restrict(u[level], b[level], tmp, b[level + 1], level)
        for _ in range(COARSE_SWEEPS - 1):
            sweep(u[LEVELS - 1], b[LEVELS - 1], LEVELS - 1)
        for level in range(LEVELS - 2, 0, -1):
            prolong_add(u[level], u[level + 1], tmp)
            sweep(u[level], b[level], level)

        rows1 = half_y * tiles_y
        planes1 = half_x * tiles_x
        start_y = half_y * tile_y - HALO // 2 + rows1
        tile = start_y // 8
        shifted = lax.rem(start_y, 8) != 0
        tile_a = pl.multiple_of(lax.rem(tile, rows1 // 8) * 8, 8)
        tile_b = pl.multiple_of(lax.rem(tile + 1, rows1 // 8) * 8, 8)
        start_x = half_x * tile_x - HALO // 2 + planes1

        def add(x0):
            parts = []
            for j in range(chunk0 // 2):
                plane = lax.rem(start_x + x0 // 2 + j, planes1)
                window = jnp.concatenate(
                    [u[1][plane, pl.ds(tile_a, 8), :], u[1][plane, pl.ds(tile_b, 8), :]], axis=0
                )
                width = half_y + HALO
                parts.append(jnp.where(shifted, window[4 : 4 + width], window[:width])[None])
            spread_add(u0, jnp.concatenate(parts, axis=0), tmp, x0, chunk0)

        over_planes(planes0, chunk0, add)

    def final_residual():
        sums = jnp.zeros((1, CY, NZ), F32)
        for part in range(CX // chunk0):
            x0 = HALO + part * chunk0
            centre, total = neighbours(u0, x0, chunk0, 0)
            res = (b0[pl.ds(x0, chunk0)] - (6.0 * centre - total)) * (1.0 / coupling)
            res = res[:, HALO : HALO + CY]
            residual_ref[pl.ds(part * chunk0, chunk0)] = res
            sums += jnp.sum(res * res, axis=0, keepdims=True)
        return jnp.sum(jnp.sum(sums[0], axis=0, keepdims=True), axis=1, keepdims=True)

    message = jnp.zeros((1, NZ), F32)
    lanes = lax.broadcasted_iota(jnp.int32, (1, NZ), 1)
    for cycle_index in range(CYCLES):
        if cycle_index == 0:
            first_sweep(u0, b0, 0)
        else:
            sweep(u0, b0, 0)
        coarse_correction(cycle_index)
        sweep(u0, b0, 0)
        message = jnp.where(lanes == cycle_index, final_residual(), message)
    norm_msg[...] = message
    potential_ref[...] = u0[HALO : HALO + CX, HALO : HALO + CY, :]
    to_all(norm_msg, norm_buf, 1 + CYCLES)
    norm_buf[me] = message
    from_all(norm_buf, 1 + CYCLES)
    totals = jnp.sum(norm_buf[...], axis=0)
    norms_ref[...] = jnp.sqrt(totals / grid_cells + norm_eps)


def per_device(tiles_x, tiles_y, particle_cell, particle_mass):
    slots = particle_cell.size
    vmem = pl.BlockSpec(memory_space=pltpu.VMEM)
    density, sums = pl.pallas_call(
        deposit_kernel,
        out_shape=(
            jax.ShapeDtypeStruct((CX * CY, NZ), F32),
            jax.ShapeDtypeStruct((1, 128), F32),
        ),
        in_specs=[vmem] * 2,
        out_specs=(vmem, vmem),
        scratch_shapes=[pltpu.VMEM((3 * CX * CY, NZ), F32), pltpu.VMEM((8, 128), F32)],
    )(particle_cell.reshape(slots // 128, 128), particle_mass.reshape(slots // 128, 128))

    count = tiles_x * tiles_y
    wide = (CX + 2 * HALO, CY + 2 * HALO, NZ)
    fields = []
    for level in range(1, LEVELS):
        shape = (CX * tiles_x >> level, CY * tiles_y >> level, NZ)
        fields += [pltpu.VMEM(shape, F32), pltpu.VMEM(shape, F32)]
    block = (CX, CY, NZ)
    tmp_rows = max(wide[1], CY * tiles_y // 2)
    potential, residual, norms = pl.pallas_call(
        functools.partial(main_kernel, tiles_x, tiles_y),
        out_shape=(
            jax.ShapeDtypeStruct(block, F32),
            jax.ShapeDtypeStruct(block, F32),
            jax.ShapeDtypeStruct((1, NZ), F32),
        ),
        in_specs=[vmem] * 2,
        out_specs=(vmem, vmem, vmem),
        scratch_shapes=[
            pltpu.VMEM(wide, F32),
            pltpu.VMEM(wide, F32),
            pltpu.VMEM(wide, F32),
            pltpu.VMEM((count, 1, NZ), F32),
            pltpu.VMEM((count, 1, NZ), F32),
            pltpu.VMEM((1, NZ), F32),
            pltpu.VMEM((CYCLES, 2, 8, NZ), F32),
            pltpu.VMEM((CYCLES, count, 2, 8, NZ), F32),
            pltpu.VMEM((16, tmp_rows, NZ), F32),
            *fields,
            pltpu.SemaphoreType.DMA((8,)),
            pltpu.SemaphoreType.DMA((8,)),
            pltpu.SemaphoreType.DMA((2 + CYCLES,)),
            pltpu.SemaphoreType.DMA((2 + CYCLES,)),
        ],
        compiler_params=pltpu.CompilerParams(collective_id=0, has_side_effects=True),
    )(density.reshape(block), sums)
    return potential, residual, norms[0, :CYCLES]


def solution(mesh):
    tiles_x, tiles_y = mesh.shape["gx"], mesh.shape["gy"]
    in_specs = (P("gx", "gy", None), P("gx", "gy", None))
    out_specs = (P("gx", "gy", None), P("gx", "gy", None), P())
    return jax.shard_map(
        functools.partial(per_device, tiles_x, tiles_y),
        mesh=mesh,
        in_specs=in_specs,
        out_specs=out_specs,
        check_vma=False,
    )
```

```python
import functools

import jax
import jax.numpy as jnp
from jax import lax
from jax.experimental import pallas as pl
from jax.experimental.pallas import tpu as pltpu
from jax.sharding import PartitionSpec as P

CX = 16
CY = 8
NZ = 128
LEVELS = 4
CYCLES = 2
COARSE_SWEEPS = 2
HALO = 8

coupling = 0.03125
norm_eps = 1e-06

MESH = pl.DeviceIdType.MESH
F32 = jnp.float32
BF16 = jnp.bfloat16


def deposit_kernel(cell_ref, mass_ref, density_ref, sums_ref, acc_ref, msum_ref):
    rows = cell_ref.shape[0]
    step = 8
    cells = CX * CY // 2
    wide = 2 * NZ
    acc_ref[...] = jnp.zeros_like(acc_ref)
    msum_ref[...] = jnp.zeros_like(msum_ref)

    def body(i, carry):
        at = pl.ds(pl.multiple_of(i * step, step), step)
        slot = cell_ref[at, :]
        mass = jnp.where(slot >= 0, mass_ref[at, :], 0.0)
        msum_ref[...] += mass
        high = mass.astype(BF16).astype(F32)
        rest = mass - high
        middle = rest.astype(BF16).astype(F32)
        low = rest - middle
        row = (slot >> 8).astype(F32)
        z = (slot & (wide - 1)).astype(F32)

        def pair(values, k):
            return jnp.broadcast_to(values[k : k + 1], (16, 128)).astype(BF16)

        ids = lax.broadcasted_iota(jnp.int32, (16, 128), 0)
        ids = [(ids + 16 * j).astype(F32).astype(BF16) for j in range(max(cells, wide) // 16)]
        one, zero = jnp.ones((16, 128), BF16), jnp.zeros((16, 128), BF16)
        left, right = [], []
        for k in range(step):
            at_row, at_z = pair(row, k), pair(z, k)
            hits = [at_row == ids[j] for j in range(cells // 16)]
            pieces = []
            for values in (high, middle, low):
                piece = pair(values, k)
                pieces += [jnp.where(hit, piece, zero) for hit in hits]
            left.append(jnp.concatenate(pieces, axis=0))
            right.append(
                jnp.concatenate([jnp.where(at_z == ids[j], one, zero) for j in range(wide // 16)], axis=0)
            )
        acc_ref[...] += lax.dot_general(
            jnp.concatenate(left, axis=1),
            jnp.concatenate(right, axis=1),
            (((1,), (1,)), ((), ())),
            preferred_element_type=F32,
        )
        return carry

    lax.fori_loop(0, rows // step, body, 0)
    density = acc_ref[0:cells] + (acc_ref[cells : 2 * cells] + acc_ref[2 * cells :])
    density_ref[pl.ds(0, cells, 2), :] = density[:, :NZ]
    density_ref[pl.ds(1, cells, 2), :] = density[:, NZ:]
    sums_ref[...] = jnp.sum(msum_ref[...], axis=0, keepdims=True)


def colour_of(shape, level):
    x = lax.broadcasted_iota(jnp.int32, shape, 0)
    y = lax.broadcasted_iota(jnp.int32, shape, 1)
    z = lax.broadcasted_iota(jnp.int32, shape, 2) >> level
    return (x + y + z) & 1


def chunk_of(planes, rows_y):
    chunk = 2
    while 2 * chunk * rows_y <= 128 and planes % (2 * chunk) == 0:
        chunk *= 2
    return chunk


def wrapped(x, planes):
    return x % planes if isinstance(x, int) else lax.rem(x, planes)


def neighbours(u_ref, x0, chunk, level):
    planes, rows_y, lanes = u_ref.shape
    centre = u_ref[pl.ds(x0, chunk)]
    if chunk == planes:
        before, after = centre[planes - 1 :], centre[:1]
    else:
        before = u_ref[pl.ds(wrapped(x0 + planes - 1, planes), 1)]
        after = u_ref[pl.ds(wrapped(x0 + chunk, planes), 1)]
    total = jnp.concatenate([before, centre[:-1]], axis=0)
    total += jnp.concatenate([centre[1:], after], axis=0)
    total += pltpu.roll(centre, 1, 1) + pltpu.roll(centre, rows_y - 1, 1)
    stride = 2**level
    total += pltpu.roll(centre, stride, 2) + pltpu.roll(centre, lanes - stride, 2)
    return centre, total


def over_planes(planes, chunk, body, start=0):
    if planes // chunk <= 8:
        for i in range(planes // chunk):
            body(start + i * chunk)
        return

    def step(i, carry):
        body(start + i * chunk)
        return carry

    lax.fori_loop(0, planes // chunk, step, 0)


def relax(u_ref, b_ref, level, wanted):
    planes, rows_y, lanes = u_ref.shape
    chunk = chunk_of(planes, rows_y)
    spacing = float(4**level)

    def body(x0):
        centre, total = neighbours(u_ref, x0, chunk, level)
        new = (total + spacing * b_ref[pl.ds(x0, chunk)]) * (1.0 / 6.0)
        u_ref[pl.ds(x0, chunk)] = jnp.where(colour_of(centre.shape, level) == wanted, new, centre)

    over_planes(planes, chunk, body)


def sweep(u_ref, b_ref, level):
    relax(u_ref, b_ref, level, 0)
    relax(u_ref, b_ref, level, 1)


def first_sweep(u_ref, b_ref, level):
    planes, rows_y, lanes = u_ref.shape
    chunk = chunk_of(planes, rows_y)
    scale = float(4**level) / 6.0

    def body(x0):
        b = b_ref[pl.ds(x0, chunk)]
        u_ref[pl.ds(x0, chunk)] = jnp.where(colour_of(b.shape, level) == 0, b * scale, 0.0)

    over_planes(planes, chunk, body)
    relax(u_ref, b_ref, level, 1)


def pair_means(u_ref, b_ref, tmp_ref, level, x0, chunk):
    centre, total = neighbours(u_ref, x0, chunk, level)
    res = b_ref[pl.ds(x0, chunk)] - (6.0 * centre - total) * (1.0 / float(4**level))
    rows_y, lanes = res.shape[1:]
    pairs = res.reshape(chunk // 2, 2, rows_y, lanes)
    along_x = pairs[:, 0] + pairs[:, 1]
    stride = 2**level
    bit = (lax.broadcasted_iota(jnp.int32, along_x.shape, 2) >> level) & 1
    other = jnp.where(
        bit == 0, pltpu.roll(along_x, lanes - stride, 2), pltpu.roll(along_x, stride, 2)
    )
    tmp_ref[0 : chunk // 2, 0:rows_y, :] = (along_x + other) * 0.125


def y_pairs(tmp_ref, count, start, rows):
    return tmp_ref[0:count, pl.ds(start, rows, 2), :] + tmp_ref[0:count, pl.ds(start + 1, rows, 2), :]


def restrict(u_ref, b_ref, tmp_ref, coarse_ref, level):
    planes, rows_y, _ = u_ref.shape
    chunk = chunk_of(planes, rows_y)

    def body(x0):
        pair_means(u_ref, b_ref, tmp_ref, level, x0, chunk)
        coarse_ref[pl.ds(x0 // 2, chunk // 2)] = y_pairs(tmp_ref, chunk // 2, 0, rows_y // 2)

    over_planes(planes, chunk, body)


def spread_add(u_ref, coarse, tmp_ref, x0, chunk):
    half, rows, lanes = coarse.shape
    tmp_ref[0:half, pl.ds(0, rows, 2), :] = coarse
    tmp_ref[0:half, pl.ds(1, rows, 2), :] = coarse
    wide = tmp_ref[0:half, 0 : 2 * rows, :]
    wide = jnp.broadcast_to(wide[:, None], (half, 2, 2 * rows, lanes))
    u_ref[pl.ds(x0, chunk)] += wide.reshape(chunk, 2 * rows, lanes)


def prolong_add(u_ref, coarse_ref, tmp_ref):
    planes, rows_y, _ = u_ref.shape
    chunk = chunk_of(planes, rows_y)

    def body(x0):
        spread_add(u_ref, coarse_ref[pl.ds(x0 // 2, chunk // 2)], tmp_ref, x0, chunk)

    over_planes(planes, chunk, body)


def main_kernel(tiles_x, tiles_y, density_ref, sums_ref, potential_ref, residual_ref, norms_ref, *scratch):
    count = tiles_x * tiles_y
    (ext, b0, u0, mass_buf, norm_buf, norm_msg, packed, gathered, tmp) = scratch[:9]
    fields = scratch[9 : 9 + 2 * (LEVELS - 1)]
    halo_send, halo_recv, all_send, all_recv, pass_send, pass_recv = scratch[9 + 2 * (LEVELS - 1) :]
    tile_x = lax.axis_index("gx")
    tile_y = lax.axis_index("gy")
    me = tile_x * tiles_y + tile_y
    side = lax.rem(tile_x, 2)
    pairs = count // 2
    my_pair = (tile_x // 2) * tiles_y + tile_y
    grid_cells = CX * CY * NZ * count
    b = [b0] + [fields[2 * i] for i in range(LEVELS - 1)]
    u = [u0] + [fields[2 * i + 1] for i in range(LEVELS - 1)]

    def partner(k):
        d = lax.rem(me + k, count)
        return (d // tiles_y, lax.rem(d, tiles_y))

    barrier = pltpu.get_barrier_semaphore()

    def greet(k, carry):
        pl.semaphore_signal(barrier, inc=1, device_id=partner(k), device_id_type=MESH)
        return carry

    lax.fori_loop(1, count, greet, 0)
    pl.semaphore_wait(barrier, count - 1)

    def to_all(src, dst, which):
        def send(k, carry):
            pltpu.make_async_remote_copy(
                src_ref=src,
                dst_ref=dst.at[me],
                send_sem=all_send.at[which],
                recv_sem=all_recv.at[which],
                device_id=partner(k),
                device_id_type=MESH,
            ).start()
            return carry

        lax.fori_loop(1, count, send, 0)

    def from_all(dst, which):
        part = dst.at[pl.ds(0, count - 1)]
        pltpu.make_async_copy(part, part, all_recv.at[which]).wait()
        pltpu.make_async_copy(part, part, all_send.at[which]).wait()

    to_all(sums_ref, mass_buf, 0)
    halos = []
    for dx, dy in ((0, 1), (0, -1), (1, 1), (-1, 1), (1, -1), (-1, -1), (1, 0), (-1, 0)):
        rows = {1: (CX - HALO, HALO, 0), 0: (0, CX, HALO), -1: (0, HALO, HALO + CX)}[dx]
        to_y = {1: 0, 0: HALO, -1: HALO + CY}[dy]
        copy = pltpu.make_async_remote_copy(
            src_ref=density_ref.at[pl.ds(rows[0], rows[1])],
            dst_ref=ext.at[pl.ds(rows[2], rows[1]), pl.ds(to_y, CY), :],
            send_sem=halo_send.at[len(halos)],
            recv_sem=halo_recv.at[len(halos)],
            device_id=(
                lax.rem(tile_x + dx + tiles_x, tiles_x),
                lax.rem(tile_y + dy + tiles_y, tiles_y),
            ),
            device_id_type=MESH,
        )
        copy.start()
        halos.append(copy)
    ext[HALO : HALO + CX, HALO : HALO + CY, :] = density_ref[...]
    mass_buf[me] = sums_ref[...]
    from_all(mass_buf, 0)
    total_mass = jnp.sum(jnp.sum(mass_buf[...], axis=0), axis=-1, keepdims=True)
    scale = coupling / (total_mass / grid_cells)
    for copy in halos:
        copy.wait()

    planes0, rows0, _ = ext.shape
    chunk0 = 4

    def set_source(x0):
        at = pl.ds(x0, chunk0)
        b0[at] = coupling - ext[at] * jnp.broadcast_to(scale.reshape(1, 1, 1), (chunk0, rows0, NZ))

    over_planes(planes0, chunk0, set_source)

    lane = lax.broadcasted_iota(jnp.int32, (1, 1, NZ), 2) & 1
    half_x, half_y = CX // 2, CY // 2

    def coarse_correction(cycle_index):
        for part in range(CX // chunk0):
            pair_means(u0, b0, tmp, 0, HALO + part * chunk0, chunk0)
            b1_part = y_pairs(tmp, chunk0 // 2, HALO, half_y)
            for j in range(chunk0 // 2):
                plane = part * (chunk0 // 2) + j
                inner = plane % 4
                at = (inner % 2, slice(half_y * (inner // 2), half_y * (inner // 2 + 1)))
                if plane < 4:
                    packed[cycle_index, at[0], at[1], :] = b1_part[j]
                else:
                    old = packed[cycle_index, at[0], at[1], :]
                    packed[cycle_index, at[0], at[1], :] = jnp.where(lane[0] == 0, old, b1_part[j])
        which = 1 + cycle_index

        def send(k, carry):
            pair = lax.rem(my_pair + k, pairs)
            pltpu.make_async_remote_copy(
                src_ref=packed.at[cycle_index],
                dst_ref=gathered.at[cycle_index, side, my_pair],
                send_sem=all_send.at[which],
                recv_sem=all_recv.at[which],
                device_id=(2 * (pair // tiles_y) + side, lax.rem(pair, tiles_y)),
                device_id_type=MESH,
            ).start()
            return carry

        lax.fori_loop(1, pairs, send, 0)
        gathered[cycle_index, side, my_pair] = packed[cycle_index]
        arrived = gathered.at[cycle_index, 0, pl.ds(0, pairs - 1)]
        pltpu.make_async_copy(arrived, arrived, all_recv.at[which]).wait()
        pltpu.make_async_copy(arrived, arrived, all_send.at[which]).wait()
        forward = pltpu.make_async_remote_copy(
            src_ref=gathered.at[cycle_index, side],
            dst_ref=gathered.at[cycle_index, side],
            send_sem=pass_send.at[cycle_index],
            recv_sem=pass_recv.at[cycle_index],
            device_id=(tile_x + 1 - 2 * side, tile_y),
            device_id_type=MESH,
        )
        forward.start()
        forward.wait()

        def unpack(ix, side_x, iy):
            pair = (ix // 2) * tiles_y + 2 * iy
            first = gathered[cycle_index, side_x, pair]
            second = gathered[cycle_index, side_x, pair + 1]
            rows = slice(iy * 8, iy * 8 + 8)
            low = jnp.concatenate([first[:, :half_y], second[:, :half_y]], axis=1)
            high = jnp.concatenate([first[:, half_y:], second[:, half_y:]], axis=1)
            for offset, part in ((0, low), (2, high)):
                even = jnp.where(lane == 0, part, pltpu.roll(part, 1, 2))
                odd = jnp.where(lane == 1, part, pltpu.roll(part, NZ - 1, 2))
                b[1][pl.ds(ix * half_x + offset, 2), rows, :] = even
                b[1][pl.ds(ix * half_x + 4 + offset, 2), rows, :] = odd

        def unpack_rows(x0):
            for side_x in range(2):
                for iy in range(tiles_y // 2):
                    unpack(x0 + side_x, side_x, iy)

        over_planes(tiles_x, 2, unpack_rows)
        for level in range(1, LEVELS):
            first_sweep(u[level], b[level], level)
            if level < LEVELS - 1:
                restrict(u[level], b[level], tmp, b[level + 1], level)
        for _ in range(COARSE_SWEEPS - 1):
            sweep(u[LEVELS - 1], b[LEVELS - 1], LEVELS - 1)
        for level in range(LEVELS - 2, 0, -1):
            prolong_add(u[level], u[level + 1], tmp)
            sweep(u[level], b[level], level)

        rows1 = half_y * tiles_y
        planes1 = half_x * tiles_x
        start_y = half_y * tile_y - HALO // 2 + rows1
        tile = start_y // 8
        shifted = lax.rem(start_y, 8) != 0
        tile_a = pl.multiple_of(lax.rem(tile, rows1 // 8) * 8, 8)
        tile_b = pl.multiple_of(lax.rem(tile + 1, rows1 // 8) * 8, 8)
        start_x = half_x * tile_x - HALO // 2 + planes1

        def add(x0):
            parts = []
            for j in range(chunk0 // 2):
                plane = lax.rem(start_x + x0 // 2 + j, planes1)
                window = jnp.concatenate(
                    [u[1][plane, pl.ds(tile_a, 8), :], u[1][plane, pl.ds(tile_b, 8), :]], axis=0
                )
                width = half_y + HALO
                parts.append(jnp.where(shifted, window[4 : 4 + width], window[:width])[None])
            spread_add(u0, jnp.concatenate(parts, axis=0), tmp, x0, chunk0)

        over_planes(planes0, chunk0, add)

    def final_residual():
        sums = jnp.zeros((1, CY, NZ), F32)
        for part in range(CX // chunk0):
            x0 = HALO + part * chunk0
            centre, total = neighbours(u0, x0, chunk0, 0)
            res = (b0[pl.ds(x0, chunk0)] - (6.0 * centre - total)) * (1.0 / coupling)
            res = res[:, HALO : HALO + CY]
            residual_ref[pl.ds(part * chunk0, chunk0)] = res
            sums += jnp.sum(res * res, axis=0, keepdims=True)
        return jnp.sum(jnp.sum(sums[0], axis=0, keepdims=True), axis=1, keepdims=True)

    message = jnp.zeros((1, NZ), F32)
    lanes = lax.broadcasted_iota(jnp.int32, (1, NZ), 1)
    for cycle_index in range(CYCLES):
        if cycle_index == 0:
            first_sweep(u0, b0, 0)
        else:
            sweep(u0, b0, 0)
        coarse_correction(cycle_index)
        sweep(u0, b0, 0)
        message = jnp.where(lanes == cycle_index, final_residual(), message)
    norm_msg[...] = message
    potential_ref[...] = u0[HALO : HALO + CX, HALO : HALO + CY, :]
    to_all(norm_msg, norm_buf, 1 + CYCLES)
    norm_buf[me] = message
    from_all(norm_buf, 1 + CYCLES)
    totals = jnp.sum(norm_buf[...], axis=0)
    norms_ref[...] = jnp.sqrt(totals / grid_cells + norm_eps)


def per_device(tiles_x, tiles_y, particle_cell, particle_mass):
    slots = particle_cell.size
    vmem = pl.BlockSpec(memory_space=pltpu.VMEM)
    density, sums = pl.pallas_call(
        deposit_kernel,
        out_shape=(
            jax.ShapeDtypeStruct((CX * CY, NZ), F32),
            jax.ShapeDtypeStruct((1, 128), F32),
        ),
        in_specs=[vmem] * 2,
        out_specs=(vmem, vmem),
        scratch_shapes=[pltpu.VMEM((3 * CX * CY // 2, 2 * NZ), F32), pltpu.VMEM((8, 128), F32)],
    )(particle_cell.reshape(slots // 128, 128), particle_mass.reshape(slots // 128, 128))

    count = tiles_x * tiles_y
    wide = (CX + 2 * HALO, CY + 2 * HALO, NZ)
    fields = []
    for level in range(1, LEVELS):
        shape = (CX * tiles_x >> level, CY * tiles_y >> level, NZ)
        fields += [pltpu.VMEM(shape, F32), pltpu.VMEM(shape, F32)]
    block = (CX, CY, NZ)
    tmp_rows = max(wide[1], CY * tiles_y // 2)
    potential, residual, norms = pl.pallas_call(
        functools.partial(main_kernel, tiles_x, tiles_y),
        out_shape=(
            jax.ShapeDtypeStruct(block, F32),
            jax.ShapeDtypeStruct(block, F32),
            jax.ShapeDtypeStruct((1, NZ), F32),
        ),
        in_specs=[vmem] * 2,
        out_specs=(vmem, vmem, vmem),
        scratch_shapes=[
            pltpu.VMEM(wide, F32),
            pltpu.VMEM(wide, F32),
            pltpu.VMEM(wide, F32),
            pltpu.VMEM((count, 1, NZ), F32),
            pltpu.VMEM((count, 1, NZ), F32),
            pltpu.VMEM((1, NZ), F32),
            pltpu.VMEM((CYCLES, 2, 8, NZ), F32),
            pltpu.VMEM((CYCLES, 2, count // 2, 2, 8, NZ), F32),
            pltpu.VMEM((16, tmp_rows, NZ), F32),
            *fields,
            pltpu.SemaphoreType.DMA((8,)),
            pltpu.SemaphoreType.DMA((8,)),
            pltpu.SemaphoreType.DMA((2 + CYCLES,)),
            pltpu.SemaphoreType.DMA((2 + CYCLES,)),
            pltpu.SemaphoreType.DMA((CYCLES,)),
            pltpu.SemaphoreType.DMA((CYCLES,)),
        ],
        compiler_params=pltpu.CompilerParams(collective_id=0, has_side_effects=True),
    )(density.reshape(block), sums)
    return potential, residual, norms[0, :CYCLES]


def solution(mesh):
    tiles_x, tiles_y = mesh.shape["gx"], mesh.shape["gy"]
    in_specs = (P("gx", "gy", None), P("gx", "gy", None))
    out_specs = (P("gx", "gy", None), P("gx", "gy", None), P())
    return jax.shard_map(
        functools.partial(per_device, tiles_x, tiles_y),
        mesh=mesh,
        in_specs=in_specs,
        out_specs=out_specs,
        check_vma=False,
    )
```
